32 devices in a mesh: dp: 4 (over z), sp: 8 (over y, x, core).
Axes of the slice: x: 2, y: 2, z: 4, core: 2. Of those that a mesh axis runs over, the one named last changes fastest.
Arguments:
- queries_in: bfloat16 [8, 8192, 16, 128], P('dp', 'sp'), may hold values from -6 to 6
- keys_in: bfloat16 [8, 8192, 16, 128], P('dp', 'sp'), may hold values from -6 to 6
- values_in: bfloat16 [8, 8192, 16, 128], P('dp', 'sp'), may hold values from -6 to 6
- out_weight: bfloat16 [2048, 2048], P('dp'), may hold values from -0.125 to 0.125
Outputs:
- block_out: bfloat16 [8, 8192, 2048], P('dp', 'sp')
The draws below stay inside these ranges and needn't reach their ends.
All inputs are finite; a program needn't handle non-finite values.
Results may differ from the reference program's by a relative error of at most 0.006.
Values may be sent and summed in bfloat16 or wider, within the bound.
No kernel may reach another device: no remote copies, remote signals or barrier semaphores. Data moves between devices by JAX's collectives and lax.ppermute only.
A program may use at most 320 MiB of HBM per device.

```python
import jax
import jax.numpy as jnp
from jax import lax

HEADS = 16
HEAD_SIZE = 128
BATCH = 8
TOKENS = 8192
WIDTH = 2048


def block_levels(own_key, dims, cuts, least, top_value):
    def one(dim, shards_of):
        draws = jax.random.uniform(jax.random.fold_in(jax.random.fold_in(own_key, 6), dim), (shards_of,), jnp.float32, least / len(cuts), top_value / len(cuts))
        return jnp.repeat(jnp.exp(draws), dims[dim] // shards_of).reshape((-1,) + (1,) * (len(dims) - dim - 1))

    gain = one(*cuts[0])
    for cut in cuts[1:]:
        gain = gain * one(*cut)
    return gain


def bell_draw(key, extent, deviation, limit, cuts=(), kind=jnp.bfloat16):
    loudness = block_levels(key, extent, cuts, -0.22, 0.18) if cuts else 1.0
    drawn = jax.random.normal(key, extent, jnp.float32) * deviation * loudness
    return jnp.minimum(jnp.maximum(drawn, -limit), limit).astype(kind)


def setup_inputs(seed: int = 0) -> dict:
    key_list = jax.random.split(jax.random.key(seed), 5)
    queries_in = bell_draw(key_list[0], (BATCH, TOKENS, HEADS, HEAD_SIZE), 1.0, 6.0, ((0, 4), (1, 8)))
    keys_in = bell_draw(key_list[1], (BATCH, TOKENS, HEADS, HEAD_SIZE), 1.0, 6.0, ((0, 4), (1, 8)))
    values_in = bell_draw(key_list[2], (BATCH, TOKENS, HEADS, HEAD_SIZE), 1.0, 6.0, ((0, 4), (1, 8)))
    out_weight = bell_draw(key_list[3], (WIDTH, WIDTH), WIDTH ** -0.5, 0.125, ((0, 4),))
    return dict(queries_in=queries_in, keys_in=keys_in, values_in=values_in, out_weight=out_weight)


def feature_map(values):
    wide = values.astype(jnp.float32)
    return (wide * wide + 0.1).astype(jnp.bfloat16)


def finish_heads(read, count):
    result = read * count ** 0.5
    return result.astype(jnp.bfloat16)


def look_up(features, state, mass):
    small = lax.optimization_barrier(state.astype(jnp.bfloat16))
    top = jnp.einsum("bthd,bhde->bthe", features.astype(jnp.float32), small.astype(jnp.float32))
    bottom = jnp.einsum("bthd,bhd->bth", features.astype(jnp.float32), mass, precision=lax.Precision.HIGHEST)
    return top / (bottom + 1e-3)[..., None]


def reference(queries_in, keys_in, values_in, out_weight):
    query_feature, key_feature = lax.optimization_barrier((feature_map(queries_in), feature_map(keys_in)))
    state = jnp.einsum("bthd,bthe->bhde", key_feature.astype(jnp.float32), values_in.astype(jnp.float32)) / TOKENS
    mass = jnp.sum(key_feature.astype(jnp.float32), axis=1) / TOKENS
    mixed = finish_heads(look_up(query_feature, state, mass), TOKENS).reshape(BATCH, TOKENS, WIDTH)
    mixed = lax.optimization_barrier(mixed)
    block_out = jnp.einsum("btw,wv->btv", mixed.astype(jnp.float32), out_weight.astype(jnp.float32)).astype(jnp.bfloat16)
    return block_out
```

```python
import functools

import jax
import jax.numpy as jnp
from jax import lax
from jax.experimental import pallas as pl
from jax.experimental.pallas import tpu as pltpu
from jax.sharding import PartitionSpec as P


PAD = 8
VMEM_BYTES = 60 * 1024 * 1024


def feature_map(values):
    wide = values.astype(jnp.float32)
    return (wide * wide + 0.1).astype(jnp.bfloat16)


def sums_kernel(half, keys, values, out, key_rows, value_rows):
    _, stretch, heads, size = keys.shape
    rows = (stretch * heads, size)
    features = feature_map(keys[0]).astype(jnp.float32)
    key_rows[...] = features.reshape(rows)
    value_rows[...] = values[0].astype(jnp.float32).reshape(rows)
    mass = jnp.sum(features, axis=0)

    @pl.when(pl.program_id(1) == 0)
    def _():
        out[...] = jnp.zeros_like(out)

    for head in range(heads):
        picked = pl.ds(head, stretch, stride=heads)
        out[0, head, :size, :] += lax.dot_general(
            key_rows[picked, :].astype(jnp.bfloat16),
            value_rows[picked, :].astype(jnp.bfloat16),
            (((0,), (0,)), ((), ())),
            preferred_element_type=jnp.float32,
        )
        out[0, head, size : size + 1, :] += mass[head : head + 1, :]


def local_sums(keys, values, half, name):
    batch, tokens, heads, size = keys.shape
    part = batch // 2
    stretch = min(tokens, 256)
    block = pl.BlockSpec((1, stretch, heads, size), lambda b, t, half: (half[0] * part + b, t, 0, 0))
    return pl.pallas_call(
        sums_kernel,
        grid_spec=pltpu.PrefetchScalarGridSpec(
            num_scalar_prefetch=1,
            grid=(part, tokens // stretch),
            in_specs=[block, block],
            out_specs=pl.BlockSpec((1, heads, size + PAD, size), lambda b, t, half: (b, 0, 0, 0)),
            scratch_shapes=[pltpu.VMEM((stretch * heads, size), jnp.float32)] * 2,
        ),
        out_shape=jax.ShapeDtypeStruct((part, heads, size + PAD, size), jnp.float32),
        compiler_params=pltpu.CompilerParams(vmem_limit_bytes=VMEM_BYTES),
        cost_estimate=pl.CostEstimate(
            flops=2 * part * tokens * heads * size * size * 4,
            bytes_accessed=4 * part * tokens * heads * size,
            transcendentals=0,
        ),
        name=name,
    )(half.reshape(1), keys, values)


def output_kernel(spot, queries, sums, own_weight, *rest, count, ranks, groups):
    pieces, (out, weight, tables, query_rows, mixed, arrived) = rest[:-6], rest[-6:]
    _, stretch, heads, size = queries.shape
    rank, group, parity = spot[0], spot[1], spot[2]
    own_rows = own_weight.shape[0]
    piece_rows = pieces[0].shape[1] if pieces else 0
    first = (pl.program_id(0) == 0) & (pl.program_id(1) == 0)

    def weight_copies():
        copies = [
            pltpu.make_async_copy(
                own_weight, weight.at[pl.ds(pl.multiple_of(rank * own_rows, own_rows), own_rows)], arrived.at[0]
            )
        ]
        for index, piece in enumerate(pieces):
            side, shift = index // groups, index % groups
            owner = 2 * ((group + groups - shift) % groups) + (parity ^ side)
            for hop in range(1, ranks):
                start = ((rank + ranks - hop) % ranks) * own_rows + owner * piece_rows
                copies.append(
                    pltpu.make_async_copy(
                        piece.at[hop - 1],
                        weight.at[pl.ds(pl.multiple_of(start, piece_rows), piece_rows)],
                        arrived.at[len(copies)],
                    )
                )
        return copies

    @pl.when(first)
    def _():
        for copy in weight_copies():
            copy.start()

    @pl.when(pl.program_id(1) == 0)
    def _():
        for head in range(heads):
            mass = sums[0, head, size : size + PAD, :].astype(jnp.float32)
            whole = jnp.broadcast_to(mass[0:1] + mass[1:2], (size, size)).T
            high = whole.astype(jnp.bfloat16)
            tables[head, :size, :size] = sums[0, head, :size, :]
            tables[head, size:, :size] = jnp.zeros((size, size), jnp.bfloat16)
            tables[head, :size, size:] = high
            tables[head, size:, size:] = (whole - high.astype(jnp.float32)).astype(jnp.bfloat16)

    query_rows[...] = feature_map(queries[0]).astype(jnp.float32).reshape(stretch * heads, size)
    for head in range(heads):
        picked = query_rows[pl.ds(head, stretch, stride=heads), :].astype(jnp.bfloat16)
        both = jnp.dot(
            jnp.concatenate([picked, picked], axis=1), tables[head], preferred_element_type=jnp.float32
        )
        read = both[:, :size] / (both[:, size:] + 0.001)
        mixed[:, head * size : (head + 1) * size] = (read * count**0.5).astype(jnp.bfloat16)

    @pl.when(first)
    def _():
        for copy in weight_copies():
            copy.wait()

    out[0] = jnp.dot(mixed[...], weight[...], preferred_element_type=jnp.float32).astype(jnp.bfloat16)


def outputs(spot, queries, sums, own_weight, pieces, count, ranks, groups):
    batch, tokens, heads, size = queries.shape
    width = own_weight.shape[1]
    part = batch // 2
    stretch = min(tokens, 256)
    anywhere = pl.BlockSpec(memory_space=pl.ANY)
    return pl.pallas_call(
        functools.partial(output_kernel, count=count, ranks=ranks, groups=groups),
        grid_spec=pltpu.PrefetchScalarGridSpec(
            num_scalar_prefetch=1,
            grid=(batch, tokens // stretch),
            in_specs=[
                pl.BlockSpec((1, stretch, heads, size), lambda b, t, spot: (b, t, 0, 0)),
                pl.BlockSpec(
                    (1, heads, size + PAD, size),
                    lambda b, t, spot: ((b // part ^ spot[2]) * part + b % part, 0, 0, 0),
                ),
                anywhere,
            ]
            + [anywhere] * len(pieces),
            out_specs=pl.BlockSpec((1, stretch, width), lambda b, t, spot: (b, t, 0)),
            scratch_shapes=[
                pltpu.VMEM((heads * size, width), jnp.bfloat16),
                pltpu.VMEM((heads, 2 * size, 2 * size), jnp.bfloat16),
                pltpu.VMEM((stretch * heads, size), jnp.float32),
                pltpu.VMEM((stretch, heads * size), jnp.bfloat16),
                pltpu.SemaphoreType.DMA((1 + len(pieces) * max(ranks - 1, 1),)),
            ],
        ),
        out_shape=jax.ShapeDtypeStruct((batch, tokens, width), jnp.bfloat16),
        compiler_params=pltpu.CompilerParams(vmem_limit_bytes=VMEM_BYTES),
        cost_estimate=pl.CostEstimate(
            flops=2 * batch * tokens * heads * size * (width + 4 * size),
            bytes_accessed=4 * batch * tokens * width + 2 * width * width,
            transcendentals=0,
        ),
        name="outputs",
    )(spot, queries, sums, own_weight, *pieces)


def shifted(value, axis, pairs):
    return lax.ppermute(value, axis, pairs)


def gather_weight(out_weight, place, ranks, devices):
    groups = devices // 2
    rows = out_weight.shape[0] // devices
    piece = lax.dynamic_slice_in_dim(out_weight, place * rows, rows, 0)
    stack = jnp.stack(
        [shifted(piece, "dp", [(r, (r + hop) % ranks) for r in range(ranks)]) for hop in range(1, ranks)]
    )
    near = [stack] + [
        shifted(stack, "sp", [(d, (d + 2 * s) % devices) for d in range(devices)]) for s in range(1, groups)
    ]
    far = [shifted(item, "sp", [(d, d ^ 1) for d in range(devices)]) for item in near]
    return near + far


def reduce_sums(kept, sent, group, devices, count):
    groups = devices // 2
    swap = [(d, d ^ 1) for d in range(devices)]
    paired = kept + shifted(sent, "sp", swap)
    part, heads, rows, size = paired.shape
    chunks = paired.reshape(groups, part * heads // groups, rows, size)

    def chunk(index):
        return lax.dynamic_index_in_dim(chunks, index % groups, 0, keepdims=False)

    total = chunk(group)
    for s in range(1, groups):
        total += shifted(chunk(group + s), "sp", [(d, (d + 2 * s) % devices) for d in range(devices)])
    total = total / count
    high = total[:, size : size + 1, :].astype(jnp.bfloat16)
    low = (total[:, size : size + 1, :] - high.astype(jnp.float32)).astype(jnp.bfloat16)
    low = jnp.pad(low, ((0, 0), (0, PAD - 2), (0, 0)))
    mine = jnp.concatenate([total[:, :size, :].astype(jnp.bfloat16), high, low], axis=1)
    whole = jnp.zeros((groups,) + mine.shape, jnp.bfloat16)
    whole = lax.dynamic_update_index_in_dim(whole, mine, group, 0)
    for s in range(1, groups):
        other = shifted(mine, "sp", [(d, (d + 2 * s) % devices) for d in range(devices)])
        whole = lax.dynamic_update_index_in_dim(whole, other, (group + groups - s) % groups, 0)
    whole = whole.reshape(paired.shape)
    return jnp.concatenate([whole, shifted(whole, "sp", swap)], axis=0)


def on_device(queries_in, keys_in, values_in, out_weight):
    devices, ranks = lax.axis_size("sp"), lax.axis_size("dp")
    place, rank = lax.axis_index("sp"), lax.axis_index("dp")
    group, parity = place // 2, place % 2
    count = queries_in.shape[1] * devices
    pieces = gather_weight(out_weight, place, ranks, devices)
    sent = local_sums(keys_in, values_in, 1 - parity, "sent_sums")
    kept = local_sums(keys_in, values_in, parity, "kept_sums")
    sums = reduce_sums(kept, sent, group, devices, count)
    spot = jnp.stack([rank, group, parity]).astype(jnp.int32)
    return outputs(spot, queries_in, sums, out_weight, pieces, count, ranks, devices // 2)


def solution(mesh):
    placed = (
        P("dp", "sp", None, None),
        P("dp", "sp", None, None),
        P("dp", "sp", None, None),
        P("dp", None),
    )
    return jax.shard_map(
        on_device, mesh=mesh, in_specs=placed, out_specs=P("dp", "sp", None), check_vma=False
    )
```
